32 devices in a mesh: gx: 4 (over z), gy: 8 (over y, x, core).
Axes of the slice: x: 2, y: 2, z: 4, core: 2. Of those that a mesh axis runs over, the one named last changes fastest.
Arguments:
- forcing: float32 [4, 512, 2048], P(None, ('gx', 'gy')), may hold values from -6 to 6
- ice_state: float32 [2, 512, 2048], P(None, ('gx', 'gy')), may hold values from 0.3 to 3, as said below
- velocity: float32 [2, 512, 2048], P(None, ('gx', 'gy')), may hold values from -4 to 4
- stress: float32 [3, 512, 2048], P(None, ('gx', 'gy')), may hold values from -4 to 4
- ice_mask: int32 [512, 2048], P(('gx', 'gy')), may hold values from 0 to 2, as said below
Outputs:
- ice_velocity: float32 [2, 512, 2048], P(None, ('gx', 'gy'))
- ice_stress: float32 [3, 512, 2048], P(None, ('gx', 'gy'))
- ocean_stress: float32 [2, 512, 2048], P(None, ('gx', 'gy'))
The draws below stay inside these ranges and needn't reach their ends.
Inputs may be any that keep to these rules, and one draw needn't show every extreme that they name: `ice_state`: row 0 lies in 0.7 to 1, row 1 in 0.3 to 3. `ice_mask`: 0 marks land, 1 open water, 2 ice-covered cells.
All inputs are finite; a program needn't handle non-finite values.
Results may differ from the reference program's by a relative error of at most 0.00002.
Values sent between devices are 32-bit elements; how exact they have to be, the bound alone decides.
A program may use at most 128 MiB of HBM per device.

```python
import math
import jax
import jax.numpy as jnp
from jax import lax

ITERS = 4
NX = 512
NY = 2048


def draw_ice_state(key, part):
    key_conc, key_thick = jax.random.split(key)
    concentration = jax.random.uniform(key_conc, (NX, NY), jnp.float32, 0.7, 1.0)
    log_thick = jax.random.uniform(key_thick, (NX, NY), jnp.float32, jnp.log(0.3), jnp.log(3.0))
    return jnp.stack([concentration, jnp.exp(log_thick)]).astype(jnp.float32)


def draw_ice_mask(key, part):
    noise = jax.random.randint(key, (NX, NY), 0, 100)
    row_index = lax.broadcasted_iota(jnp.int32, (NX, NY), 1)
    polar_band = jnp.abs(2 * row_index - NY + 1) * 100 // NY
    return jnp.where(noise >= 95, 0, jnp.where(noise < 50 + polar_band // 3, 2, 1)).astype(jnp.int32)


def block_scale(key, dims, shards, low, high):
    def one(dim, parts):
        heights = jax.random.uniform(jax.random.fold_in(jax.random.fold_in(key, 6), dim), (parts,), jnp.float32, low / len(shards), high / len(shards))
        return jnp.repeat(jnp.exp(heights), dims[dim] // parts).reshape((-1,) + (1,) * (len(dims) - dim - 1))

    gain = one(*shards[0])
    for cut in shards[1:]:
        gain = gain * one(*cut)
    return gain


def bell_draw(key, shape, width, limit, cuts=(), kind=jnp.bfloat16):
    values = width * jax.random.normal(key, shape, jnp.float32)
    if cuts:
        values = values * block_scale(key, shape, cuts, -0.22, 0.18)
    return jnp.clip(values, -limit, limit).astype(kind)


def setup_inputs(seed: int = 0) -> dict:
    seeds = jax.random.split(jax.random.key(seed), 6)
    forcing = bell_draw(seeds[0], (4, NX, NY), 1.0, 6.0, ((1, 32),), jnp.float32)
    ice_state = draw_ice_state(jax.random.fold_in(seeds[5], 71), 0)
    velocity = bell_draw(seeds[2], (2, NX, NY), 0.5, 4.0, ((1, 32),), jnp.float32)
    stress = bell_draw(seeds[3], (3, NX, NY), 0.5, 4.0, ((1, 32),), jnp.float32)
    ice_mask = draw_ice_mask(jax.random.fold_in(seeds[5], 71), 0)
    return dict(forcing=forcing, ice_state=ice_state, velocity=velocity, stress=stress, ice_mask=ice_mask)


P_STAR = 1.0
C_STAR = 20.0
ECC_SQ = 4.0
DELTA_MIN = 0.05
ALPHA_EVP = 30.0
BETA_EVP = 30.0
DRAG_COEF = 0.5
SPEED_FLOOR = 0.05
CORIOLIS_MAX = 0.5

def extend_global(fields, sign_flip):
    top_row = fields[:, ::-1, -1:] * sign_flip[:, None, None]
    tall = jnp.concatenate([jnp.zeros_like(top_row), fields, top_row], axis=2)
    return jnp.concatenate([tall[:, -1:, :], tall, tall[:, :1, :]], axis=1)

def update_stress(vel_ext, state, pressure, ice_cover):
    u_field = vel_ext[0]
    v_field = vel_ext[1]
    diff_u = u_field[1:, 1:] - u_field[:-1, 1:]
    diff_v = v_field[1:, 1:] - v_field[1:, :-1]
    divergence = diff_u + diff_v
    tension = diff_u - diff_v
    shear_all = u_field[:-1, 1:] - u_field[:-1, :-1] + v_field[1:, :-1] - v_field[:-1, :-1]
    shear_cell = 0.25 * (shear_all[1:, 1:] + shear_all[:-1, 1:] + shear_all[1:, :-1] + shear_all[:-1, :-1])
    div_cell = divergence[:-1, :-1]
    ten_cell = tension[:-1, :-1]
    delta_cell = jnp.sqrt(div_cell * div_cell + (ten_cell * ten_cell + shear_cell * shear_cell) / ECC_SQ)
    capped = delta_cell + DELTA_MIN
    target_one = pressure * (div_cell - delta_cell) / capped
    target_two = pressure * ten_cell / (ECC_SQ * capped)
    div_corner = 0.25 * (divergence[:-1, :-1] + divergence[1:, :-1] + divergence[:-1, 1:] + divergence[1:, 1:])
    ten_corner = 0.25 * (tension[:-1, :-1] + tension[1:, :-1] + tension[:-1, 1:] + tension[1:, 1:])
    shear_corner = shear_all[1:, 1:]
    delta_corner = jnp.sqrt(div_corner * div_corner + (ten_corner * ten_corner + shear_corner * shear_corner) / ECC_SQ)
    capped_corner = delta_corner + DELTA_MIN
    target_three = pressure * shear_corner / (2.0 * ECC_SQ * capped_corner)
    targets = jnp.stack([target_one, target_two, target_three])
    return ice_cover[None] * (state + (targets - state) / ALPHA_EVP)

def update_velocity(vel_ext, stress_ext, start_vel, currents, wind_stress, ice_mass, coriolis, ice_cover, open_water):
    sigma_one = stress_ext[0]
    sigma_two = stress_ext[1]
    sigma_shear = stress_ext[2]
    normal_xx = 0.5 * (sigma_one + sigma_two)
    normal_yy = 0.5 * (sigma_one - sigma_two)
    force_u = normal_xx[2:, 1:-1] - normal_xx[1:-1, 1:-1] + sigma_shear[1:-1, 1:-1] - sigma_shear[1:-1, :-2]
    force_v = normal_yy[1:-1, 2:] - normal_yy[1:-1, 1:-1] + sigma_shear[1:-1, 1:-1] - sigma_shear[:-2, 1:-1]
    u_field = vel_ext[0]
    v_field = vel_ext[1]
    u_now = u_field[1:-1, 1:-1]
    v_now = v_field[1:-1, 1:-1]
    v_at_u = 0.25 * (v_field[1:-1, 1:-1] + v_field[2:, 1:-1] + v_field[1:-1, :-2] + v_field[2:, :-2])
    u_at_v = 0.25 * (u_field[1:-1, 1:-1] + u_field[:-2, 1:-1] + u_field[1:-1, 2:] + u_field[:-2, 2:])
    drag_u = DRAG_COEF * jnp.sqrt((currents[0] - u_now) ** 2 + SPEED_FLOOR ** 2)
    drag_v = DRAG_COEF * jnp.sqrt((currents[1] - v_now) ** 2 + SPEED_FLOOR ** 2)
    u_new = (BETA_EVP * u_now + start_vel[0] + (force_u + wind_stress[0] + drag_u * currents[0]) / ice_mass + coriolis * v_at_u) / (BETA_EVP + 1.0 + drag_u / ice_mass)
    v_new = (BETA_EVP * v_now + start_vel[1] + (force_v + wind_stress[1] + drag_v * currents[1]) / ice_mass - coriolis * u_at_v) / (BETA_EVP + 1.0 + drag_v / ice_mass)
    fresh = jnp.stack([u_new, v_new])
    return ice_cover[None] * fresh + open_water[None] * currents

def coriolis_field(first_row, row_count, total_rows):
    row_index = (first_row + jnp.arange(row_count, dtype=jnp.int32)).astype(jnp.float32)
    latitude = math.pi * ((row_index + 0.5) / total_rows - 0.5)
    return CORIOLIS_MAX * jnp.sin(latitude)[None, :]

def run_window(forcing, ice_state, velocity, stress, ice_mask, extend, first_row, total_rows):
    concentration = ice_state[0]
    thickness = ice_state[1]
    pressure = P_STAR * thickness * jnp.exp(-C_STAR * (1.0 - concentration))
    ice_mass = concentration * thickness
    ice_cover = (ice_mask == 2).astype(jnp.float32)
    open_water = (ice_mask == 1).astype(jnp.float32)
    currents = forcing[0:2]
    wind_stress = forcing[2:4]
    coriolis = coriolis_field(first_row, ice_mask.shape[1], total_rows)
    vel_flip = jnp.array([-1.0, -1.0], jnp.float32)
    stress_flip = jnp.array([1.0, 1.0, 1.0], jnp.float32)
    current_vel = velocity
    state = stress
    for turn_index in range(ITERS):
        vel_ext = extend(current_vel, vel_flip)
        state = update_stress(vel_ext, state, pressure, ice_cover)
        stress_ext = extend(state, stress_flip)
        current_vel = update_velocity(vel_ext, stress_ext, velocity, currents, wind_stress, ice_mass, coriolis, ice_cover, open_water)
    drag_final = DRAG_COEF * jnp.sqrt((currents - current_vel) ** 2 + SPEED_FLOOR ** 2)
    ocean = drag_final * (current_vel - currents)
    return (current_vel, state, ocean)

def reference(forcing, ice_state, velocity, stress, ice_mask):
    return run_window(forcing, ice_state, velocity, stress, ice_mask, extend_global, 0, NY)
```

```python
import functools
import math

import jax
import jax.numpy as jnp
from jax import lax
from jax.experimental import pallas as pl
from jax.experimental.pallas import tpu as pltpu
from jax.sharding import PartitionSpec as P

ITERS = 4
C_STAR = 20.0
DELTA_MIN = 0.05
ALPHA_EVP = 30.0
BETA_EVP = 30.0
DRAG_COEF = 0.5
SPEED_FLOOR = 0.05
CORIOLIS_MAX = 0.5

MESH = pl.DeviceIdType.MESH
LANES = 128
SUB = 8
OFF = 7
CH = 2
VEL_HALO = 6
REST_HALO = 5
STRESS_REACH = (5, 4, 2, 1)
VEL_REACH = (5, 3, 2, 0)


def loop(lo, hi, body):
    turns = (hi - lo) // CH

    def turn(t, carry):
        body(lo + t * CH)
        return carry

    lax.fori_loop(0, turns, turn, 0)


def drag(current, speed):
    gap = current - speed
    return DRAG_COEF * jnp.sqrt(gap * gap + SPEED_FLOOR**2)


def statics(conc, thick, kind, un, vn, tx, ty, uo, vo):
    ice = jnp.where(kind == 2.0, 1.0, 0.0).astype(jnp.float32)
    open_water = jnp.where(kind == 1.0, 1.0, 0.0).astype(jnp.float32)
    push = ice * (thick * jnp.exp(-C_STAR * (1.0 - conc))) * (1.0 / ALPHA_EVP)
    inv_mass = 1.0 / (conc * thick)
    return (
        push,
        ice,
        inv_mass,
        un + tx * inv_mass,
        vn + ty * inv_mass,
        open_water * uo,
        open_water * vo,
    )


KEEP = 1.0 - 1.0 / ALPHA_EVP


def stress_rule(s1, s2, s12, div, ten, shear4, div4, ten4, shear, push, ice):
    delta = jnp.sqrt(div * div + 0.25 * (ten * ten) + (1.0 / 64.0) * (shear4 * shear4))
    rate = push / (delta + DELTA_MIN)
    delta_k = jnp.sqrt(
        (1.0 / 16.0) * (div4 * div4 + 0.25 * (ten4 * ten4)) + 0.25 * (shear * shear)
    )
    rate_k = push / (delta_k + DELTA_MIN)
    keep = KEEP * ice
    return (
        keep * s1 + rate * (div - delta),
        keep * s2 + rate * (0.25 * ten),
        keep * s12 + rate_k * (0.125 * shear),
    )


def vel_rule(now, start, force, cur, inv_mass, turn, ice, water):
    w = drag(cur, now)
    top = BETA_EVP * now + start + (force + w * cur) * inv_mass + turn
    return ice * (top / (BETA_EVP + 1.0 + w * inv_mass)) + water


def kernel(
    n_gx, n_gy, forcing, ice_state, velocity, stress, kinds,
    out_vel, out_stress, out_ocean,
    nat_f, nat_i, nat_v, nat_s, nat_k, res_v, res_s, res_o,
    V, S, X, ST, UP, DN, SDN, NUP, cor,
    tile, MP, MV, MS, MST, MN, G, GN,
    in_sem, out_sem, send_sem, recv_sem, msend_sem, mrecv_sem,
):
    count = n_gx * n_gy
    me = lax.axis_index("gx") * n_gy + lax.axis_index("gy")
    cols = kinds.shape[0] * SUB
    rows = V.shape[3]
    total_rows = rows * LANES
    flip_base = cols + SUB - 1
    mrows = cols + 2 * SUB

    def device(q):
        return (q // n_gy, q % n_gy)

    left = (me + count - 1) % count
    right = (me + 1) % count
    mirror = count - 1 - me
    mir_l = (2 * count - 2 - me) % count
    mir_r = (count - me) % count

    loads = [
        pltpu.make_async_copy(a, b, in_sem.at[t])
        for t, (a, b) in enumerate(
            ((velocity, nat_v), (kinds, nat_k), (stress, nat_s), (ice_state, nat_i), (forcing, nat_f))
        )
    ]
    for c in loads:
        c.start()

    barrier = pltpu.get_barrier_semaphore()
    for q in (left, right, mirror):
        pl.semaphore_signal(barrier, inc=1, device_id=device(q), device_id_type=MESH)

    @pl.when(mir_l != me)
    def _():
        pl.semaphore_signal(barrier, inc=1, device_id=device(mir_l), device_id_type=MESH)

    @pl.when(mir_r != me)
    def _():
        pl.semaphore_signal(barrier, inc=1, device_id=device(mir_r), device_id_type=MESH)

    row_i = lax.broadcasted_iota(jnp.int32, (rows, LANES), 0)
    lane_i = lax.broadcasted_iota(jnp.int32, (rows, LANES), 1)
    lat = math.pi * (((row_i * LANES + lane_i).astype(jnp.float32) + 0.5) / total_rows - 0.5)
    cor[...] = CORIOLIS_MAX * jnp.sin(lat)

    for c in loads:
        c.wait()

    lane_t = lax.broadcasted_iota(jnp.int32, (SUB, LANES), 1)
    fields = (
        [(nat_v, f) for f in range(2)]
        + [(nat_s, f) for f in range(3)]
        + [(nat_f, f) for f in range(4)]
        + [(nat_i, f) for f in range(2)]
        + [(nat_k, None)]
    )
    last = (rows - 1) * SUB
    for b in range(cols // SUB):
        packed = jnp.zeros((SUB, LANES), jnp.float32)
        for f, (ref, g) in enumerate(fields):
            part = ref[b, last : last + SUB, :] if g is None else ref[g, b, last : last + SUB, :]
            part = part.astype(jnp.float32)
            part = pltpu.roll(part, (SUB * f + SUB) % LANES, 1)
            packed = jnp.where((lane_t >= SUB * f) & (lane_t < SUB * f + SUB), part, packed)
        tile[b * SUB : b * SUB + SUB, :] = packed

    for b in range(cols // SUB):

        def spread(r, carry):
            w = OFF + b * SUB + r
            at = pl.ds(r, rows, stride=SUB)
            for f in range(2):
                V[0, f, w] = nat_v[f, b, at, :]
            for f in range(3):
                S[0, f, w] = nat_s[f, b, at, :]
            for f in range(4):
                X[f, w] = nat_f[f, b, at, :]
            for f in range(2):
                X[4 + f, w] = nat_i[f, b, at, :]
            X[6, w] = nat_k[b, at, :].astype(jnp.float32)
            return carry

        lax.fori_loop(0, SUB, spread, 0)

    own_l, own_r = OFF, OFF + cols

    pl.semaphore_wait(
        barrier, 5 - jnp.where(mir_l == me, 1, 0) - jnp.where(mir_r == me, 1, 0)
    )

    def remote(src, dst, ssem, rsem, q):
        return pltpu.make_async_remote_copy(
            src_ref=src, dst_ref=dst, send_sem=ssem, recv_sem=rsem,
            device_id=device(q), device_id_type=MESH,
        )

    to_mirror = remote(
        tile, MP.at[pl.ds(SUB, cols)], msend_sem.at[0], mrecv_sem.at[0], mirror
    )
    to_ml = remote(
        tile.at[pl.ds(cols - SUB, SUB)], MP.at[pl.ds(0, SUB)], msend_sem.at[1], mrecv_sem.at[1], mir_l
    )
    to_mr = remote(
        tile.at[pl.ds(0, SUB)], MP.at[pl.ds(SUB + cols, SUB)], msend_sem.at[2], mrecv_sem.at[2], mir_r
    )
    to_mirror.start()

    @pl.when(mir_l != me)
    def _():
        to_ml.start()

    @pl.when(mir_r != me)
    def _():
        to_mr.start()

    sends = []
    for t, (buf, halo) in enumerate(((V.at[0], VEL_HALO), (S.at[0], REST_HALO), (X, REST_HALO))):
        sends.append(
            remote(
                buf.at[:, pl.ds(own_l, halo)], buf.at[:, pl.ds(own_r, halo)],
                send_sem.at[2 * t], recv_sem.at[2 * t], left,
            )
        )
        sends.append(
            remote(
                buf.at[:, pl.ds(own_r - halo, halo)], buf.at[:, pl.ds(own_l - halo, halo)],
                send_sem.at[2 * t + 1], recv_sem.at[2 * t + 1], right,
            )
        )
    for c in sends:
        c.start()

    def prepare(c):
        w = pl.ds(c + OFF, CH)
        got = statics(
            X[4, w], X[5, w], X[6, w], V[0, 0, w], V[0, 1, w], X[2, w], X[3, w], X[0, w], X[1, w]
        )
        for f, value in enumerate(got):
            ST[f, w] = value

    loop(0, cols, prepare)

    lane_e = lax.broadcasted_iota(jnp.int32, (rows, LANES), 1)
    row_e = lax.broadcasted_iota(jnp.int32, (rows, LANES), 0)
    at_last = lane_e == LANES - 1
    at_first = lane_e == 0
    at_top = at_last & (row_e == rows - 1)
    at_bottom = at_first & (row_e == 0)

    def shift_up(x, ghost):
        r = pltpu.roll(x, LANES - 1, 1)
        q = pltpu.roll(r, rows - 1, 0)
        return jnp.where(at_top, ghost, jnp.where(at_last, q, r))

    def shift_down(x):
        r = pltpu.roll(x, 1, 1)
        q = pltpu.roll(r, 1, 0)
        return jnp.where(at_bottom, 0.0, jnp.where(at_first, q, r))

    def put_shifts(k, c, j, u, v):
        w = c + OFF + j
        slot = pl.ds(flip_base - c - j, 1)
        UP[k, 0, w] = shift_up(u, -MV[k, 0, slot, :])
        UP[k, 1, w] = shift_up(v, -MV[k, 1, slot, :])
        DN[k, 0, w] = shift_down(u)
        DN[k, 1, w] = shift_down(v)
        G[k, 0, slot, :] = u[rows - 1 : rows, :]
        G[k, 1, slot, :] = v[rows - 1 : rows, :]

    def shift_start(c):
        for j in range(CH):
            put_shifts(0, c, j, V[0, 0, c + OFF + j], V[0, 1, c + OFF + j])

    def stress_step(k, c):
        wide = pl.ds(c + OFF - 1, CH + 2)
        w = pl.ds(c + OFF, CH)
        u, v = V[k, 0, wide], V[k, 1, wide]
        up, vp = UP[k, 0, wide], UP[k, 1, wide]
        um, vm = DN[k, 0, wide], DN[k, 1, wide]
        du = u[1:] - u[:-1]
        dup = up[1:] - up[:-1]
        dv = v[1:] - vm[1:]
        dvp = vp[1:] - v[1:]
        div = du + dv
        ten = du - dv
        dsum = div + (dup + dvp)
        tsum = ten + (dup - dvp)
        shear = (up[:-1] - u[:-1]) + (v[1:] - v[:-1])
        ssum = shear + ((u[:-1] - um[:-1]) + (vm[1:] - vm[:-1]))
        s1, s2, s12 = stress_rule(
            S[k, 0, w], S[k, 1, w], S[k, 2, w],
            div[:-1], ten[:-1], ssum[1:] + ssum[:-1],
            dsum[1:] + dsum[:-1], tsum[1:] + tsum[:-1], shear[1:],
            ST[0, w], ST[1, w],
        )
        S[k + 1, 0, w] = s1
        S[k + 1, 1, w] = s2
        S[k + 1, 2, w] = s12
        n22 = s1 - s2
        for j in range(CH):
            slot = pl.ds(flip_base - c - j, 1)
            SDN[k, c + OFF + j] = shift_down(s12[j])
            NUP[k, c + OFF + j] = shift_up(n22[j], MN[slot, :])
            GN[k, slot, :] = n22[j, rows - 1 : rows, :]

    def vel_step(k, c):
        w = pl.ds(c + OFF, CH)
        nxt = pl.ds(c + OFF, CH + 1)
        prv = pl.ds(c + OFF - 1, CH + 1)
        sr1, sr2 = S[k + 1, 0, nxt], S[k + 1, 1, nxt]
        s12 = S[k + 1, 2, prv]
        n11 = sr1 + sr2
        n22 = sr1[:-1] - sr2[:-1]
        fu = 0.5 * (n11[1:] - n11[:-1]) + (s12[1:] - SDN[k, w])
        fv = 0.5 * (NUP[k, w] - n22) + (s12[1:] - s12[:-1])
        v = V[k, 1, nxt]
        u = V[k, 0, prv]
        va = v + DN[k, 1, nxt]
        ua = u + UP[k, 0, prv]
        f = 0.25 * cor[...][None]
        ice, inv_mass = ST[1, w], ST[2, w]
        uo, vo = X[0, w], X[1, w]
        un = vel_rule(u[1:], ST[3, w], fu, uo, inv_mass, f * (va[1:] + va[:-1]), ice, ST[5, w])
        vn = vel_rule(v[:-1], ST[4, w], fv, vo, inv_mass, -f * (ua[1:] + ua[:-1]), ice, ST[6, w])
        if k + 1 < ITERS:
            V[k + 1, 0, w] = un
            V[k + 1, 1, w] = vn
            for j in range(CH):
                put_shifts(k + 1, c, j, un[j], vn[j])
            return
        ou = drag(uo, un) * (un - uo)
        ov = drag(vo, vn) * (vn - vo)
        for j in range(CH):
            b, r = c // SUB, c % SUB + j
            at = pl.ds(r, rows, stride=SUB)
            res_v[0, b, at, :] = un[j]
            res_v[1, b, at, :] = vn[j]
            res_s[0, b, at, :] = sr1[j]
            res_s[1, b, at, :] = sr2[j]
            res_s[2, b, at, :] = s12[j + 1]
            res_o[0, b, at, :] = ou[j]
            res_o[1, b, at, :] = ov[j]

    lane_m = lax.broadcasted_iota(jnp.int32, (mrows, LANES), 1)
    m_last = lane_m == LANES - 1

    def m_west(x):
        return pltpu.roll(x, 1, 0)

    def m_east(x):
        return pltpu.roll(x, mrows - 1, 0)

    def m_down(x):
        return pltpu.roll(x, 1, 1)

    def m_up(x, ghost):
        return jnp.where(m_last, ghost, pltpu.roll(x, LANES - 1, 1))

    def m_prepare():
        whole = MP[...]
        raw = [
            whole if (LANES - SUB - SUB * f) % LANES == 0
            else pltpu.roll(whole, (LANES - SUB - SUB * f) % LANES, 1)
            for f in range(12)
        ]
        u, v, s1, s2, s12, uo, vo, tx, ty, conc, thick, kind = raw
        MV[0, 0], MV[0, 1] = u, v
        MS[0], MS[1], MS[2] = s1, s2, s12
        for f, value in enumerate(statics(conc, thick, kind, u, v, tx, ty, uo, vo)):
            MST[f] = value
        MST[7] = uo
        MST[8] = vo

    def m_stress(k):
        u, v = MV[k, 0], MV[k, 1]
        up, vp = m_up(u, -G[k, 0]), m_up(v, -G[k, 1])
        um, vm = m_down(u), m_down(v)
        du = u - m_west(u)
        dup = up - m_west(up)
        dv = v - vm
        dvp = vp - v
        div, ten = du + dv, du - dv
        dsum, tsum = div + (dup + dvp), ten + (dup - dvp)
        shear = (up - u) + (m_east(v) - v)
        ssum = shear + ((u - um) + (m_east(vm) - vm))
        src = 3 * k
        got = stress_rule(
            MS[src], MS[src + 1], MS[src + 2], div, ten, ssum + m_west(ssum),
            dsum + m_east(dsum), tsum + m_east(tsum), shear, MST[0], MST[1],
        )
        for f in range(3):
            MS[src + 3 + f] = got[f]
        MN[...] = got[0] - got[1]

    def m_vel(k):
        src = 3 * k + 3
        s1, s2, s12 = MS[src], MS[src + 1], MS[src + 2]
        n11, n22 = s1 + s2, s1 - s2
        u, v = MV[k, 0], MV[k, 1]
        up, vm = m_up(u, -G[k, 0]), m_down(v)
        fu = 0.5 * (m_east(n11) - n11) + (s12 - m_down(s12))
        fv = 0.5 * (m_up(n22, GN[k]) - n22) + (s12 - m_west(s12))
        va, ua = v + vm, u + up
        f = 0.25 * cor[rows - 1 : rows, :]
        MV[k + 1, 0] = vel_rule(
            u, MST[3], fu, MST[7], MST[2], f * (va + m_east(va)), MST[1], MST[5]
        )
        MV[k + 1, 1] = vel_rule(
            v, MST[4], fv, MST[8], MST[2], -f * (ua + m_west(ua)), MST[1], MST[6]
        )

    to_mirror.wait_recv()

    @pl.when(mir_l != me)
    def _():
        to_ml.wait_recv()

    @pl.when(mir_l == me)
    def _():
        MP[0:SUB, :] = tile[cols - SUB : cols, :]

    @pl.when(mir_r != me)
    def _():
        to_mr.wait_recv()

    @pl.when(mir_r == me)
    def _():
        MP[SUB + cols : mrows, :] = tile[0:SUB, :]

    m_prepare()

    def sweep(start_parts, stress_parts, vel_parts):
        for lo, hi in start_parts:
            loop(lo, hi, shift_start)
        for k in range(len(stress_parts)):
            m_stress(k)
            for lo, hi in stress_parts[k]:
                loop(lo, hi, functools.partial(stress_step, k))
            if k + 1 < ITERS:
                m_vel(k)
                for lo, hi in vel_parts[k]:
                    loop(lo, hi, functools.partial(vel_step, k))

    inner = (1, 4, 6)
    inner_vel = (3, 5, 8)
    sweep(
        [(0, cols)],
        [[(a, cols - a)] for a in inner],
        [[(a, cols - a)] for a in inner_vel],
    )

    for c in sends:
        c.wait_recv()

    loop(-VEL_HALO, 0, shift_start)
    loop(cols, cols + VEL_HALO, shift_start)
    edge = REST_HALO + 1
    loop(-edge, 0, prepare)
    loop(cols, cols + edge, prepare)

    def both(reach, a):
        return [(-reach, a), (cols - a, cols + reach)]

    sweep(
        [],
        [both(r, a) for r, a in zip(STRESS_REACH[:3], inner)]
        + [[(-STRESS_REACH[3], cols + STRESS_REACH[3])]],
        [both(r, a) for r, a in zip(VEL_REACH[:2], inner_vel)]
        + [[(-VEL_REACH[2], cols + VEL_REACH[2])]],
    )

    outs = []
    for b in range(cols // SUB):
        for c in range(b * SUB, (b + 1) * SUB, CH):
            vel_step(ITERS - 1, c)
        for t, (src, dst) in enumerate(((res_v, out_vel), (res_s, out_stress), (res_o, out_ocean))):
            outs.append(
                pltpu.make_async_copy(src.at[:, b], dst.at[:, b], out_sem.at[3 * b + t])
            )
            outs[-1].start()

    to_mirror.wait_send()

    @pl.when(mir_l != me)
    def _():
        to_ml.wait_send()

    @pl.when(mir_r != me)
    def _():
        to_mr.wait_send()

    for c in sends:
        c.wait_send()
    for c in outs:
        c.wait()


def to_tiles(x):
    lead, (c, r) = x.shape[:-2], x.shape[-2:]
    x = x.reshape(lead + (c // SUB, SUB, r // LANES, LANES))
    return jnp.swapaxes(x, -3, -2).reshape(lead + (c // SUB, r // LANES * SUB, LANES))


def from_tiles(x, c, r):
    lead = x.shape[:-3]
    x = x.reshape(lead + (c // SUB, r // LANES, SUB, LANES))
    return jnp.swapaxes(x, -3, -2).reshape(lead + (c, r))


def on_device(n_gx, n_gy, forcing, ice_state, velocity, stress, ice_mask):
    cols, height = ice_mask.shape
    rows = height // LANES
    blocks = cols // SUB
    width = cols + 2 * OFF
    f32 = jnp.float32

    def tiles(n):
        return (n, blocks, rows * SUB, LANES)

    def vmem(*shape):
        return pltpu.VMEM(shape, f32)

    mrows = cols + 2 * SUB
    dma = pltpu.SemaphoreType.DMA
    scratch = [
        vmem(*tiles(4)), vmem(*tiles(2)), vmem(*tiles(2)), vmem(*tiles(3)),
        pltpu.VMEM(tiles(1)[1:], jnp.int32),
        vmem(*tiles(2)), vmem(*tiles(3)), vmem(*tiles(2)),
        vmem(ITERS, 2, width, rows, LANES),
        vmem(ITERS + 1, 3, width, rows, LANES),
        vmem(7, width, rows, LANES),
        vmem(7, width, rows, LANES),
        vmem(ITERS, 2, width, rows, LANES),
        vmem(ITERS, 2, width, rows, LANES),
        vmem(ITERS, width, rows, LANES),
        vmem(ITERS, width, rows, LANES),
        vmem(rows, LANES),
        vmem(cols, LANES),
        vmem(mrows, LANES),
        vmem(ITERS, 2, mrows, LANES),
        vmem(3 * (ITERS + 1), mrows, LANES),
        vmem(9, mrows, LANES),
        vmem(mrows, LANES),
        vmem(ITERS, 2, mrows, LANES),
        vmem(ITERS, mrows, LANES),
        dma((5,)), dma((3 * blocks,)), dma((6,)), dma((6,)), dma((3,)), dma((3,)),
    ]
    any_spec = pl.BlockSpec(memory_space=pl.ANY)
    vel, str_, ocean = pl.pallas_call(
        functools.partial(kernel, n_gx, n_gy),
        out_shape=[jax.ShapeDtypeStruct(tiles(n), f32) for n in (2, 3, 2)],
        in_specs=[any_spec] * 5,
        out_specs=[any_spec] * 3,
        scratch_shapes=scratch,
        compiler_params=pltpu.CompilerParams(
            collective_id=0, has_side_effects=True, vmem_limit_bytes=60 * 1024 * 1024
        ),
    )(to_tiles(forcing), to_tiles(ice_state), to_tiles(velocity), to_tiles(stress), to_tiles(ice_mask))
    return (
        from_tiles(vel, cols, height),
        from_tiles(str_, cols, height),
        from_tiles(ocean, cols, height),
    )


def solution(mesh):
    spec = P(None, ("gx", "gy"), None)
    return jax.shard_map(
        functools.partial(on_device, mesh.shape["gx"], mesh.shape["gy"]),
        mesh=mesh,
        in_specs=(spec, spec, spec, spec, P(("gx", "gy"), None)),
        out_specs=(spec, spec, spec),
        check_vma=False,
    )
```

```python
import functools
import math

import jax
import jax.numpy as jnp
from jax import lax
from jax.experimental import pallas as pl
from jax.experimental.pallas import tpu as pltpu
from jax.sharding import PartitionSpec as P

ITERS = 4
C_STAR = 20.0
DELTA_MIN = 0.05
ALPHA_EVP = 30.0
BETA_EVP = 30.0
DRAG_COEF = 0.5
SPEED_FLOOR = 0.05
CORIOLIS_MAX = 0.5

MESH = pl.DeviceIdType.MESH
LANES = 128
SUB = 8
OFF = 7
CH = 2
VEL_HALO = 6
REST_HALO = 5
STRESS_REACH = (5, 4, 2, 1)
VEL_REACH = (5, 3, 2, 0)


def loop(lo, hi, body):
    half = (hi - lo) // (2 * CH)
    pairs(lo, hi - half * CH, half, body)
    if (hi - lo) // CH > 2 * half:
        body([lo + half * CH])


def pairs(lo, other, turns, body):
    def turn(t, carry):
        body([lo + t * CH, other + t * CH])
        return carry

    lax.fori_loop(0, turns, turn, 0)


def drag(current, speed):
    gap = current - speed
    return DRAG_COEF * jnp.sqrt(gap * gap + SPEED_FLOOR**2)


def statics(conc, thick, kind, un, vn, tx, ty, uo, vo):
    ice = jnp.where(kind == 2.0, 1.0, 0.0).astype(jnp.float32)
    open_water = jnp.where(kind == 1.0, 1.0, 0.0).astype(jnp.float32)
    push = ice * (thick * jnp.exp(-C_STAR * (1.0 - conc))) * (1.0 / ALPHA_EVP)
    inv_mass = 1.0 / (conc * thick)
    return (
        push,
        ice,
        inv_mass,
        un + tx * inv_mass,
        vn + ty * inv_mass,
        open_water * uo,
        open_water * vo,
    )


KEEP = 1.0 - 1.0 / ALPHA_EVP


def stress_rule(s1, s2, s12, div, ten, shear4, div4, ten4, shear, push, ice):
    delta = jnp.sqrt(div * div + 0.25 * (ten * ten) + (1.0 / 64.0) * (shear4 * shear4))
    rate = push / (delta + DELTA_MIN)
    delta_k = jnp.sqrt(
        (1.0 / 16.0) * (div4 * div4 + 0.25 * (ten4 * ten4)) + 0.25 * (shear * shear)
    )
    rate_k = push / (delta_k + DELTA_MIN)
    keep = KEEP * ice
    return (
        keep * s1 + rate * (div - delta),
        keep * s2 + rate * (0.25 * ten),
        keep * s12 + rate_k * (0.125 * shear),
    )


def vel_rule(now, start, force, cur, inv_mass, turn, ice, water):
    w = drag(cur, now)
    top = BETA_EVP * now + start + (force + w * cur) * inv_mass + turn
    return ice * (top / (BETA_EVP + 1.0 + w * inv_mass)) + water


def kernel(
    n_gx, n_gy, nat_f, nat_i, nat_v, nat_s, nat_k,
    res_v, res_s, res_o,
    V, S, X, ST, UP, DN, SDN, NUP, cor,
    tile, MP, MV, MS, MST, MN, G, GN,
    send_sem, recv_sem, msend_sem, mrecv_sem,
):
    count = n_gx * n_gy
    me = lax.axis_index("gx") * n_gy + lax.axis_index("gy")
    cols = nat_k.shape[0] * SUB
    rows = V.shape[3]
    total_rows = rows * LANES
    flip_base = cols + SUB - 1
    mrows = cols + 2 * SUB

    def device(q):
        return (q // n_gy, q % n_gy)

    left = (me + count - 1) % count
    right = (me + 1) % count
    mirror = count - 1 - me
    mir_l = (2 * count - 2 - me) % count
    mir_r = (count - me) % count

    barrier = pltpu.get_barrier_semaphore()
    for q in (left, right, mirror):
        pl.semaphore_signal(barrier, inc=1, device_id=device(q), device_id_type=MESH)

    @pl.when(mir_l != me)
    def _():
        pl.semaphore_signal(barrier, inc=1, device_id=device(mir_l), device_id_type=MESH)

    @pl.when(mir_r != me)
    def _():
        pl.semaphore_signal(barrier, inc=1, device_id=device(mir_r), device_id_type=MESH)

    row_i = lax.broadcasted_iota(jnp.int32, (rows, LANES), 0)
    lane_i = lax.broadcasted_iota(jnp.int32, (rows, LANES), 1)
    lat = math.pi * (((row_i * LANES + lane_i).astype(jnp.float32) + 0.5) / total_rows - 0.5)
    cor[...] = CORIOLIS_MAX * jnp.sin(lat)

    lane_t = lax.broadcasted_iota(jnp.int32, (SUB, LANES), 1)
    fields = (
        [(nat_v, f) for f in range(2)]
        + [(nat_s, f) for f in range(3)]
        + [(nat_f, f) for f in range(4)]
        + [(nat_i, f) for f in range(2)]
        + [(nat_k, None)]
    )
    last = (rows - 1) * SUB
    for b in range(cols // SUB):
        packed = jnp.zeros((SUB, LANES), jnp.float32)
        for f, (ref, g) in enumerate(fields):
            part = ref[b, last : last + SUB, :] if g is None else ref[g, b, last : last + SUB, :]
            part = part.astype(jnp.float32)
            part = pltpu.roll(part, (SUB * f + SUB) % LANES, 1)
            packed = jnp.where((lane_t >= SUB * f) & (lane_t < SUB * f + SUB), part, packed)
        tile[b * SUB : b * SUB + SUB, :] = packed

    for b in range(cols // SUB):

        def spread(r, carry):
            w = OFF + b * SUB + r
            at = pl.ds(r, rows, stride=SUB)
            for f in range(2):
                V[0, f, w] = nat_v[f, b, at, :]
            for f in range(3):
                S[0, f, w] = nat_s[f, b, at, :]
            for f in range(4):
                X[f, w] = nat_f[f, b, at, :]
            for f in range(2):
                X[4 + f, w] = nat_i[f, b, at, :]
            X[6, w] = nat_k[b, at, :].astype(jnp.float32)
            return carry

        lax.fori_loop(0, SUB, spread, 0)

    own_l, own_r = OFF, OFF + cols

    pl.semaphore_wait(
        barrier, 5 - jnp.where(mir_l == me, 1, 0) - jnp.where(mir_r == me, 1, 0)
    )

    def remote(src, dst, ssem, rsem, q):
        return pltpu.make_async_remote_copy(
            src_ref=src, dst_ref=dst, send_sem=ssem, recv_sem=rsem,
            device_id=device(q), device_id_type=MESH,
        )

    to_mirror = remote(
        tile, MP.at[pl.ds(SUB, cols)], msend_sem.at[0], mrecv_sem.at[0], mirror
    )
    to_ml = remote(
        tile.at[pl.ds(cols - SUB, SUB)], MP.at[pl.ds(0, SUB)], msend_sem.at[1], mrecv_sem.at[1], mir_l
    )
    to_mr = remote(
        tile.at[pl.ds(0, SUB)], MP.at[pl.ds(SUB + cols, SUB)], msend_sem.at[2], mrecv_sem.at[2], mir_r
    )
    to_mirror.start()

    @pl.when(mir_l != me)
    def _():
        to_ml.start()

    @pl.when(mir_r != me)
    def _():
        to_mr.start()

    sends = []
    for t, (buf, halo) in enumerate(((V.at[0], VEL_HALO), (S.at[0], REST_HALO), (X, REST_HALO))):
        sends.append(
            remote(
                buf.at[:, pl.ds(own_l, halo)], buf.at[:, pl.ds(own_r, halo)],
                send_sem.at[2 * t], recv_sem.at[2 * t], left,
            )
        )
        sends.append(
            remote(
                buf.at[:, pl.ds(own_r - halo, halo)], buf.at[:, pl.ds(own_l - halo, halo)],
                send_sem.at[2 * t + 1], recv_sem.at[2 * t + 1], right,
            )
        )
    for c in sends:
        c.start()

    def prepare(cs):
        for c in cs:
            prepare_pair(c)

    def prepare_pair(c):
        w = pl.ds(c + OFF, CH)
        got = statics(
            X[4, w], X[5, w], X[6, w], V[0, 0, w], V[0, 1, w], X[2, w], X[3, w], X[0, w], X[1, w]
        )
        for f, value in enumerate(got):
            ST[f, w] = value

    loop(0, cols, prepare)

    lane_e = lax.broadcasted_iota(jnp.int32, (rows, LANES), 1)
    row_e = lax.broadcasted_iota(jnp.int32, (rows, LANES), 0)
    at_last = lane_e == LANES - 1
    at_first = lane_e == 0
    at_top = at_last & (row_e == rows - 1)
    at_bottom = at_first & (row_e == 0)

    def shift_up(x, ghost):
        r = pltpu.roll(x, LANES - 1, 1)
        q = pltpu.roll(r, rows - 1, 0)
        return jnp.where(at_top, ghost, jnp.where(at_last, q, r))

    def shift_down(x):
        r = pltpu.roll(x, 1, 1)
        q = pltpu.roll(r, 1, 0)
        return jnp.where(at_bottom, 0.0, jnp.where(at_first, q, r))

    def put_shifts(k, c, j, u, v):
        w = c + OFF + j
        slot = pl.ds(flip_base - c - j, 1)
        UP[k, 0, w] = shift_up(u, -MV[k, 0, slot, :])
        UP[k, 1, w] = shift_up(v, -MV[k, 1, slot, :])
        DN[k, 0, w] = shift_down(u)
        DN[k, 1, w] = shift_down(v)
        G[k, 0, slot, :] = u[rows - 1 : rows, :]
        G[k, 1, slot, :] = v[rows - 1 : rows, :]

    def shift_start(cs):
        got = [
            (c, j, V[0, 0, c + OFF + j], V[0, 1, c + OFF + j]) for c in cs for j in range(CH)
        ]
        for c, j, u, v in got:
            put_shifts(0, c, j, u, v)

    def stress_step(k, cs):
        got = [stress_of(k, c) for c in cs]
        for c, (s1, s2, s12) in zip(cs, got):
            put_stress(k, c, s1, s2, s12)

    def stress_of(k, c):
        wide = pl.ds(c + OFF - 1, CH + 2)
        w = pl.ds(c + OFF, CH)
        u, v = V[k, 0, wide], V[k, 1, wide]
        up, vp = UP[k, 0, wide], UP[k, 1, wide]
        um, vm = DN[k, 0, wide], DN[k, 1, wide]
        du = u[1:] - u[:-1]
        dup = up[1:] - up[:-1]
        dv = v[1:] - vm[1:]
        dvp = vp[1:] - v[1:]
        div = du + dv
        ten = du - dv
        dsum = div + (dup + dvp)
        tsum = ten + (dup - dvp)
        shear = (up[:-1] - u[:-1]) + (v[1:] - v[:-1])
        ssum = shear + ((u[:-1] - um[:-1]) + (vm[1:] - vm[:-1]))
        return stress_rule(
            S[k, 0, w], S[k, 1, w], S[k, 2, w],
            div[:-1], ten[:-1], ssum[1:] + ssum[:-1],
            dsum[1:] + dsum[:-1], tsum[1:] + tsum[:-1], shear[1:],
            ST[0, w], ST[1, w],
        )

    def put_stress(k, c, s1, s2, s12):
        w = pl.ds(c + OFF, CH)
        ups, downs = [], []
        n22 = s1 - s2
        for j in range(CH):
            slot = pl.ds(flip_base - c - j, 1)
            downs.append(shift_down(s12[j]))
            ups.append(shift_up(n22[j], MN[slot, :]))
        S[k + 1, 0, w] = s1
        S[k + 1, 1, w] = s2
        S[k + 1, 2, w] = s12
        for j in range(CH):
            slot = pl.ds(flip_base - c - j, 1)
            SDN[k, c + OFF + j] = downs[j]
            NUP[k, c + OFF + j] = ups[j]
            GN[k, slot, :] = n22[j, rows - 1 : rows, :]

    def vel_step(k, cs):
        got = [vel_of(k, c) for c in cs]
        for c, values in zip(cs, got):
            put_vel(k, c, *values)

    def vel_of(k, c):
        w = pl.ds(c + OFF, CH)
        nxt = pl.ds(c + OFF, CH + 1)
        prv = pl.ds(c + OFF - 1, CH + 1)
        sr1, sr2 = S[k + 1, 0, nxt], S[k + 1, 1, nxt]
        s12 = S[k + 1, 2, prv]
        n11 = sr1 + sr2
        n22 = sr1[:-1] - sr2[:-1]
        fu = 0.5 * (n11[1:] - n11[:-1]) + (s12[1:] - SDN[k, w])
        fv = 0.5 * (NUP[k, w] - n22) + (s12[1:] - s12[:-1])
        v = V[k, 1, nxt]
        u = V[k, 0, prv]
        va = v + DN[k, 1, nxt]
        ua = u + UP[k, 0, prv]
        f = 0.25 * cor[...][None]
        ice, inv_mass = ST[1, w], ST[2, w]
        uo, vo = X[0, w], X[1, w]
        un = vel_rule(u[1:], ST[3, w], fu, uo, inv_mass, f * (va[1:] + va[:-1]), ice, ST[5, w])
        vn = vel_rule(v[:-1], ST[4, w], fv, vo, inv_mass, -f * (ua[1:] + ua[:-1]), ice, ST[6, w])
        return un, vn, uo, vo, sr1, sr2, s12

    def put_vel(k, c, un, vn, uo, vo, sr1, sr2, s12):
        w = pl.ds(c + OFF, CH)
        if k + 1 < ITERS:
            V[k + 1, 0, w] = un
            V[k + 1, 1, w] = vn
            for j in range(CH):
                put_shifts(k + 1, c, j, un[j], vn[j])
            return
        ou = drag(uo, un) * (un - uo)
        ov = drag(vo, vn) * (vn - vo)
        for j in range(CH):
            b, r = c // SUB, c % SUB + j
            at = pl.ds(r, rows, stride=SUB)
            res_v[0, b, at, :] = un[j]
            res_v[1, b, at, :] = vn[j]
            res_s[0, b, at, :] = sr1[j]
            res_s[1, b, at, :] = sr2[j]
            res_s[2, b, at, :] = s12[j + 1]
            res_o[0, b, at, :] = ou[j]
            res_o[1, b, at, :] = ov[j]

    lane_m = lax.broadcasted_iota(jnp.int32, (mrows, LANES), 1)
    m_last = lane_m == LANES - 1

    def m_west(x):
        return pltpu.roll(x, 1, 0)

    def m_east(x):
        return pltpu.roll(x, mrows - 1, 0)

    def m_down(x):
        return pltpu.roll(x, 1, 1)

    def m_up(x, ghost):
        return jnp.where(m_last, ghost, pltpu.roll(x, LANES - 1, 1))

    def m_prepare():
        whole = MP[...]
        raw = [
            whole if (LANES - SUB - SUB * f) % LANES == 0
            else pltpu.roll(whole, (LANES - SUB - SUB * f) % LANES, 1)
            for f in range(12)
        ]
        u, v, s1, s2, s12, uo, vo, tx, ty, conc, thick, kind = raw
        MV[0, 0], MV[0, 1] = u, v
        MS[0], MS[1], MS[2] = s1, s2, s12
        for f, value in enumerate(statics(conc, thick, kind, u, v, tx, ty, uo, vo)):
            MST[f] = value
        MST[7] = uo
        MST[8] = vo

    def m_stress(k):
        u, v = MV[k, 0], MV[k, 1]
        up, vp = m_up(u, -G[k, 0]), m_up(v, -G[k, 1])
        um, vm = m_down(u), m_down(v)
        du = u - m_west(u)
        dup = up - m_west(up)
        dv = v - vm
        dvp = vp - v
        div, ten = du + dv, du - dv
        dsum, tsum = div + (dup + dvp), ten + (dup - dvp)
        shear = (up - u) + (m_east(v) - v)
        ssum = shear + ((u - um) + (m_east(vm) - vm))
        src = 3 * k
        got = stress_rule(
            MS[src], MS[src + 1], MS[src + 2], div, ten, ssum + m_west(ssum),
            dsum + m_east(dsum), tsum + m_east(tsum), shear, MST[0], MST[1],
        )
        for f in range(3):
            MS[src + 3 + f] = got[f]
        MN[...] = got[0] - got[1]

    def m_vel(k):
        src = 3 * k + 3
        s1, s2, s12 = MS[src], MS[src + 1], MS[src + 2]
        n11, n22 = s1 + s2, s1 - s2
        u, v = MV[k, 0], MV[k, 1]
        up, vm = m_up(u, -G[k, 0]), m_down(v)
        fu = 0.5 * (m_east(n11) - n11) + (s12 - m_down(s12))
        fv = 0.5 * (m_up(n22, GN[k]) - n22) + (s12 - m_west(s12))
        va, ua = v + vm, u + up
        f = 0.25 * cor[rows - 1 : rows, :]
        MV[k + 1, 0] = vel_rule(
            u, MST[3], fu, MST[7], MST[2], f * (va + m_east(va)), MST[1], MST[5]
        )
        MV[k + 1, 1] = vel_rule(
            v, MST[4], fv, MST[8], MST[2], -f * (ua + m_west(ua)), MST[1], MST[6]
        )

    to_mirror.wait_recv()

    @pl.when(mir_l != me)
    def _():
        to_ml.wait_recv()

    @pl.when(mir_l == me)
    def _():
        MP[0:SUB, :] = tile[cols - SUB : cols, :]

    @pl.when(mir_r != me)
    def _():
        to_mr.wait_recv()

    @pl.when(mir_r == me)
    def _():
        MP[SUB + cols : mrows, :] = tile[0:SUB, :]

    m_prepare()

    def run(part, body):
        if len(part) == 3:
            pairs(*part, body)
        else:
            loop(*part, body)

    def sweep(start_parts, stress_parts, vel_parts):
        for lo, hi in start_parts:
            loop(lo, hi, shift_start)
        for k in range(len(stress_parts)):
            m_stress(k)
            for part in stress_parts[k]:
                run(part, functools.partial(stress_step, k))
            if k + 1 < ITERS:
                m_vel(k)
                for part in vel_parts[k]:
                    run(part, functools.partial(vel_step, k))

    inner = (1, 4, 6)
    inner_vel = (3, 5, 8)
    sweep(
        [(0, cols)],
        [[(a, cols - a)] for a in inner],
        [[(a, cols - a)] for a in inner_vel],
    )

    for c in sends:
        c.wait_recv()

    pairs(-VEL_HALO, cols, VEL_HALO // CH, shift_start)
    edge = REST_HALO + 1
    pairs(-edge, cols, edge // CH, prepare)

    def both(reach, a):
        return [(-reach, cols - a, (reach + a) // CH)]

    sweep(
        [],
        [both(r, a) for r, a in zip(STRESS_REACH[:3], inner)]
        + [[(-STRESS_REACH[3], cols + STRESS_REACH[3])]],
        [both(r, a) for r, a in zip(VEL_REACH[:2], inner_vel)]
        + [[(-VEL_REACH[2], cols + VEL_REACH[2])]],
    )

    for c in range(0, cols, 2 * CH):
        vel_step(ITERS - 1, [c, c + CH])

    to_mirror.wait_send()

    @pl.when(mir_l != me)
    def _():
        to_ml.wait_send()

    @pl.when(mir_r != me)
    def _():
        to_mr.wait_send()

    for c in sends:
        c.wait_send()

def write_out(a, b, c, out_a, out_b, out_c, sem):
    copies = [
        pltpu.make_async_copy(src, dst, sem.at[t])
        for t, (src, dst) in enumerate(((b, out_b), (a, out_a), (c, out_c)))
    ]
    for copy in copies:
        copy.start()
    for copy in copies:
        copy.wait()


def to_tiles(x):
    lead, (c, r) = x.shape[:-2], x.shape[-2:]
    x = x.reshape(lead + (c // SUB, SUB, r // LANES, LANES))
    return jnp.swapaxes(x, -3, -2).reshape(lead + (c // SUB, r // LANES * SUB, LANES))


def from_tiles(x, c, r):
    lead = x.shape[:-3]
    x = x.reshape(lead + (c // SUB, r // LANES, SUB, LANES))
    return jnp.swapaxes(x, -3, -2).reshape(lead + (c, r))


def on_device(n_gx, n_gy, forcing, ice_state, velocity, stress, ice_mask):
    cols, height = ice_mask.shape
    rows = height // LANES
    blocks = cols // SUB
    width = cols + 2 * OFF
    f32 = jnp.float32

    def tiles(n):
        return (n, blocks, rows * SUB, LANES)

    def vmem(*shape):
        return pltpu.VMEM(shape, f32)

    mrows = cols + 2 * SUB
    dma = pltpu.SemaphoreType.DMA
    scratch = [
        vmem(ITERS, 2, width, rows, LANES),
        vmem(ITERS + 1, 3, width, rows, LANES),
        vmem(7, width, rows, LANES),
        vmem(7, width, rows, LANES),
        vmem(ITERS, 2, width, rows, LANES),
        vmem(ITERS, 2, width, rows, LANES),
        vmem(ITERS, width, rows, LANES),
        vmem(ITERS, width, rows, LANES),
        vmem(rows, LANES),
        vmem(cols, LANES),
        vmem(mrows, LANES),
        vmem(ITERS, 2, mrows, LANES),
        vmem(3 * (ITERS + 1), mrows, LANES),
        vmem(9, mrows, LANES),
        vmem(mrows, LANES),
        vmem(ITERS, 2, mrows, LANES),
        vmem(ITERS, mrows, LANES),
        dma((6,)), dma((6,)), dma((3,)), dma((3,)),
    ]
    any_spec = pl.BlockSpec(memory_space=pltpu.HBM)
    vmem_spec = pl.BlockSpec(memory_space=pltpu.VMEM)
    shapes = [jax.ShapeDtypeStruct(tiles(n), f32) for n in (2, 3, 2)]
    results = pl.pallas_call(
        functools.partial(kernel, n_gx, n_gy),
        out_shape=shapes,
        in_specs=[vmem_spec] * 5,
        out_specs=[vmem_spec] * 3,
        scratch_shapes=scratch,
        compiler_params=pltpu.CompilerParams(
            collective_id=0, has_side_effects=True, vmem_limit_bytes=44 * 1024 * 1024
        ),
    )(to_tiles(forcing), to_tiles(ice_state), to_tiles(velocity), to_tiles(stress), to_tiles(ice_mask))
    vel, str_, ocean = pl.pallas_call(
        write_out,
        out_shape=shapes,
        in_specs=[vmem_spec] * 3,
        out_specs=[any_spec] * 3,
        scratch_shapes=[dma((3,))],
        compiler_params=pltpu.CompilerParams(vmem_limit_bytes=8 * 1024 * 1024),
    )(*results)
    return (
        from_tiles(vel, cols, height),
        from_tiles(str_, cols, height),
        from_tiles(ocean, cols, height),
    )


def solution(mesh):
    spec = P(None, ("gx", "gy"), None)
    return jax.shard_map(
        functools.partial(on_device, mesh.shape["gx"], mesh.shape["gy"]),
        mesh=mesh,
        in_specs=(spec, spec, spec, spec, P(("gx", "gy"), None)),
        out_specs=(spec, spec, spec),
        check_vma=False,
    )
```

```python
import functools
import math

import jax
import jax.numpy as jnp
from jax import lax
from jax.experimental import pallas as pl
from jax.experimental.pallas import tpu as pltpu
from jax.sharding import PartitionSpec as P

ITERS = 4
C_STAR = 20.0
DELTA_MIN = 0.05
ALPHA_EVP = 30.0
BETA_EVP = 30.0
DRAG_COEF = 0.5
SPEED_FLOOR = 0.05
CORIOLIS_MAX = 0.5

MESH = pl.DeviceIdType.MESH
LANES = 128
SUB = 8
OFF = 7
CH = 2
VEL_HALO = 6
REST_HALO = 5
STRESS_REACH = (5, 4, 2, 1)
VEL_REACH = (5, 3, 2, 0)


def loop(lo, hi, body):
    half = (hi - lo) // (2 * CH)
    pairs(lo, hi - half * CH, half, body)
    if (hi - lo) // CH > 2 * half:
        body([lo + half * CH])


def pairs(lo, other, turns, body):
    def turn(t, carry):
        body([lo + t * CH, other + t * CH])
        return carry

    lax.fori_loop(0, turns, turn, 0)


def drag(current, speed):
    gap = current - speed
    return DRAG_COEF * jnp.sqrt(gap * gap + SPEED_FLOOR**2)


def statics(conc, thick, kind, un, vn, tx, ty, uo, vo):
    ice = jnp.where(kind == 2.0, 1.0, 0.0).astype(jnp.float32)
    open_water = jnp.where(kind == 1.0, 1.0, 0.0).astype(jnp.float32)
    push = ice * (thick * jnp.exp(-C_STAR * (1.0 - conc))) * (1.0 / ALPHA_EVP)
    inv_mass = 1.0 / (conc * thick)
    return (
        push,
        ice,
        inv_mass,
        un + tx * inv_mass,
        vn + ty * inv_mass,
        open_water * uo,
        open_water * vo,
    )


KEEP = 1.0 - 1.0 / ALPHA_EVP


def stress_rule(s1, s2, s12, div, ten, shear4, div4, ten4, shear, push, ice):
    delta = jnp.sqrt(div * div + 0.25 * (ten * ten) + (1.0 / 64.0) * (shear4 * shear4))
    rate = push / (delta + DELTA_MIN)
    delta_k = jnp.sqrt(
        (1.0 / 16.0) * (div4 * div4 + 0.25 * (ten4 * ten4)) + 0.25 * (shear * shear)
    )
    rate_k = push / (delta_k + DELTA_MIN)
    keep = KEEP * ice
    return (
        keep * s1 + rate * (div - delta),
        keep * s2 + rate * (0.25 * ten),
        keep * s12 + rate_k * (0.125 * shear),
    )


def vel_rule(now, start, force, cur, inv_mass, turn, ice, water):
    w = drag(cur, now)
    top = BETA_EVP * now + start + (force + w * cur) * inv_mass + turn
    return ice * (top / (BETA_EVP + 1.0 + w * inv_mass)) + water


def kernel(
    n_gx, n_gy, forcing, ice_state, velocity, stress, kinds,
    out_vel, out_stress, out_ocean,
    nat_f, nat_i, nat_v, nat_s, nat_k, res_v, res_s, res_o,
    V, S, X, ST, UP, DN, SDN, NUP, cor,
    tile, MP, MV, MS, MST, MN, G, GN,
    in_sem, out_sem, send_sem, recv_sem, msend_sem, mrecv_sem,
):
    count = n_gx * n_gy
    me = lax.axis_index("gx") * n_gy + lax.axis_index("gy")
    cols = kinds.shape[0] * SUB
    rows = V.shape[3]
    total_rows = rows * LANES
    flip_base = cols + SUB - 1
    mrows = cols + 2 * SUB

    def device(q):
        return (q // n_gy, q % n_gy)

    left = (me + count - 1) % count
    right = (me + 1) % count
    mirror = count - 1 - me
    mir_l = (2 * count - 2 - me) % count
    mir_r = (count - me) % count

    loads = [
        pltpu.make_async_copy(a, b, in_sem.at[t])
        for t, (a, b) in enumerate(
            ((velocity, nat_v), (kinds, nat_k), (stress, nat_s), (ice_state, nat_i), (forcing, nat_f))
        )
    ]
    for c in loads:
        c.start()

    barrier = pltpu.get_barrier_semaphore()
    for q in (left, right, mirror):
        pl.semaphore_signal(barrier, inc=1, device_id=device(q), device_id_type=MESH)

    @pl.when(mir_l != me)
    def _():
        pl.semaphore_signal(barrier, inc=1, device_id=device(mir_l), device_id_type=MESH)

    @pl.when(mir_r != me)
    def _():
        pl.semaphore_signal(barrier, inc=1, device_id=device(mir_r), device_id_type=MESH)

    row_i = lax.broadcasted_iota(jnp.int32, (rows, LANES), 0)
    lane_i = lax.broadcasted_iota(jnp.int32, (rows, LANES), 1)
    lat = math.pi * (((row_i * LANES + lane_i).astype(jnp.float32) + 0.5) / total_rows - 0.5)
    cor[...] = CORIOLIS_MAX * jnp.sin(lat)

    for c in loads:
        c.wait()

    lane_t = lax.broadcasted_iota(jnp.int32, (SUB, LANES), 1)
    fields = (
        [(nat_v, f) for f in range(2)]
        + [(nat_s, f) for f in range(3)]
        + [(nat_f, f) for f in range(4)]
        + [(nat_i, f) for f in range(2)]
        + [(nat_k, None)]
    )
    last = (rows - 1) * SUB
    for b in range(cols // SUB):
        packed = jnp.zeros((SUB, LANES), jnp.float32)
        for f, (ref, g) in enumerate(fields):
            part = ref[b, last : last + SUB, :] if g is None else ref[g, b, last : last + SUB, :]
            part = part.astype(jnp.float32)
            part = pltpu.roll(part, (SUB * f + SUB) % LANES, 1)
            packed = jnp.where((lane_t >= SUB * f) & (lane_t < SUB * f + SUB), part, packed)
        tile[b * SUB : b * SUB + SUB, :] = packed

    for b in range(cols // SUB):

        def spread(r, carry):
            w = OFF + b * SUB + r
            at = pl.ds(r, rows, stride=SUB)
            for f in range(2):
                V[0, f, w] = nat_v[f, b, at, :]
            for f in range(3):
                S[0, f, w] = nat_s[f, b, at, :]
            for f in range(4):
                X[f, w] = nat_f[f, b, at, :]
            for f in range(2):
                X[4 + f, w] = nat_i[f, b, at, :]
            X[6, w] = nat_k[b, at, :].astype(jnp.float32)
            return carry

        lax.fori_loop(0, SUB, spread, 0)

    own_l, own_r = OFF, OFF + cols

    pl.semaphore_wait(
        barrier, 5 - jnp.where(mir_l == me, 1, 0) - jnp.where(mir_r == me, 1, 0)
    )

    def remote(src, dst, ssem, rsem, q):
        return pltpu.make_async_remote_copy(
            src_ref=src, dst_ref=dst, send_sem=ssem, recv_sem=rsem,
            device_id=device(q), device_id_type=MESH,
        )

    to_mirror = remote(
        tile, MP.at[pl.ds(SUB, cols)], msend_sem.at[0], mrecv_sem.at[0], mirror
    )
    to_ml = remote(
        tile.at[pl.ds(cols - SUB, SUB)], MP.at[pl.ds(0, SUB)], msend_sem.at[1], mrecv_sem.at[1], mir_l
    )
    to_mr = remote(
        tile.at[pl.ds(0, SUB)], MP.at[pl.ds(SUB + cols, SUB)], msend_sem.at[2], mrecv_sem.at[2], mir_r
    )
    to_mirror.start()

    @pl.when(mir_l != me)
    def _():
        to_ml.start()

    @pl.when(mir_r != me)
    def _():
        to_mr.start()

    sends = []
    for t, (buf, halo) in enumerate(((V.at[0], VEL_HALO), (S.at[0], REST_HALO), (X, REST_HALO))):
        sends.append(
            remote(
                buf.at[:, pl.ds(own_l, halo)], buf.at[:, pl.ds(own_r, halo)],
                send_sem.at[2 * t], recv_sem.at[2 * t], left,
            )
        )
        sends.append(
            remote(
                buf.at[:, pl.ds(own_r - halo, halo)], buf.at[:, pl.ds(own_l - halo, halo)],
                send_sem.at[2 * t + 1], recv_sem.at[2 * t + 1], right,
            )
        )
    for c in sends:
        c.start()

    def prepare(cs):
        for c in cs:
            prepare_pair(c)

    def prepare_pair(c):
        w = pl.ds(c + OFF, CH)
        got = statics(
            X[4, w], X[5, w], X[6, w], V[0, 0, w], V[0, 1, w], X[2, w], X[3, w], X[0, w], X[1, w]
        )
        for f, value in enumerate(got):
            ST[f, w] = value

    loop(0, cols, prepare)

    lane_e = lax.broadcasted_iota(jnp.int32, (rows, LANES), 1)
    row_e = lax.broadcasted_iota(jnp.int32, (rows, LANES), 0)
    at_last = lane_e == LANES - 1
    at_first = lane_e == 0
    at_top = at_last & (row_e == rows - 1)
    at_bottom = at_first & (row_e == 0)

    def shift_up(x, ghost):
        r = pltpu.roll(x, LANES - 1, 1)
        q = pltpu.roll(r, rows - 1, 0)
        return jnp.where(at_top, ghost, jnp.where(at_last, q, r))

    def shift_down(x):
        r = pltpu.roll(x, 1, 1)
        q = pltpu.roll(r, 1, 0)
        return jnp.where(at_bottom, 0.0, jnp.where(at_first, q, r))

    def put_shifts(k, c, j, u, v):
        w = c + OFF + j
        slot = pl.ds(flip_base - c - j, 1)
        UP[k, 0, w] = shift_up(u, -MV[k, 0, slot, :])
        UP[k, 1, w] = shift_up(v, -MV[k, 1, slot, :])
        DN[k, 0, w] = shift_down(u)
        DN[k, 1, w] = shift_down(v)
        G[k, 0, slot, :] = u[rows - 1 : rows, :]
        G[k, 1, slot, :] = v[rows - 1 : rows, :]

    def shift_start(cs):
        got = [
            (c, j, V[0, 0, c + OFF + j], V[0, 1, c + OFF + j]) for c in cs for j in range(CH)
        ]
        for c, j, u, v in got:
            put_shifts(0, c, j, u, v)

    def stress_step(k, cs):
        got = [stress_of(k, c) for c in cs]
        for c, (s1, s2, s12) in zip(cs, got):
            put_stress(k, c, s1, s2, s12)

    def stress_of(k, c):
        wide = pl.ds(c + OFF - 1, CH + 2)
        w = pl.ds(c + OFF, CH)
        u, v = V[k, 0, wide], V[k, 1, wide]
        up, vp = UP[k, 0, wide], UP[k, 1, wide]
        um, vm = DN[k, 0, wide], DN[k, 1, wide]
        du = u[1:] - u[:-1]
        dup = up[1:] - up[:-1]
        dv = v[1:] - vm[1:]
        dvp = vp[1:] - v[1:]
        div = du + dv
        ten = du - dv
        dsum = div + (dup + dvp)
        tsum = ten + (dup - dvp)
        shear = (up[:-1] - u[:-1]) + (v[1:] - v[:-1])
        ssum = shear + ((u[:-1] - um[:-1]) + (vm[1:] - vm[:-1]))
        return stress_rule(
            S[k, 0, w], S[k, 1, w], S[k, 2, w],
            div[:-1], ten[:-1], ssum[1:] + ssum[:-1],
            dsum[1:] + dsum[:-1], tsum[1:] + tsum[:-1], shear[1:],
            ST[0, w], ST[1, w],
        )

    def put_stress(k, c, s1, s2, s12):
        w = pl.ds(c + OFF, CH)
        ups, downs = [], []
        n22 = s1 - s2
        for j in range(CH):
            slot = pl.ds(flip_base - c - j, 1)
            downs.append(shift_down(s12[j]))
            ups.append(shift_up(n22[j], MN[slot, :]))
        S[k + 1, 0, w] = s1
        S[k + 1, 1, w] = s2
        S[k + 1, 2, w] = s12
        for j in range(CH):
            slot = pl.ds(flip_base - c - j, 1)
            SDN[k, c + OFF + j] = downs[j]
            NUP[k, c + OFF + j] = ups[j]
            GN[k, slot, :] = n22[j, rows - 1 : rows, :]

    def vel_step(k, cs):
        got = [vel_of(k, c) for c in cs]
        for c, values in zip(cs, got):
            put_vel(k, c, *values)

    def vel_of(k, c):
        w = pl.ds(c + OFF, CH)
        nxt = pl.ds(c + OFF, CH + 1)
        prv = pl.ds(c + OFF - 1, CH + 1)
        sr1, sr2 = S[k + 1, 0, nxt], S[k + 1, 1, nxt]
        s12 = S[k + 1, 2, prv]
        n11 = sr1 + sr2
        n22 = sr1[:-1] - sr2[:-1]
        fu = 0.5 * (n11[1:] - n11[:-1]) + (s12[1:] - SDN[k, w])
        fv = 0.5 * (NUP[k, w] - n22) + (s12[1:] - s12[:-1])
        v = V[k, 1, nxt]
        u = V[k, 0, prv]
        va = v + DN[k, 1, nxt]
        ua = u + UP[k, 0, prv]
        f = 0.25 * cor[...][None]
        ice, inv_mass = ST[1, w], ST[2, w]
        uo, vo = X[0, w], X[1, w]
        un = vel_rule(u[1:], ST[3, w], fu, uo, inv_mass, f * (va[1:] + va[:-1]), ice, ST[5, w])
        vn = vel_rule(v[:-1], ST[4, w], fv, vo, inv_mass, -f * (ua[1:] + ua[:-1]), ice, ST[6, w])
        return un, vn, uo, vo, sr1, sr2, s12

    def put_vel(k, c, un, vn, uo, vo, sr1, sr2, s12):
        w = pl.ds(c + OFF, CH)
        if k + 1 < ITERS:
            V[k + 1, 0, w] = un
            V[k + 1, 1, w] = vn
            for j in range(CH):
                put_shifts(k + 1, c, j, un[j], vn[j])
            return
        ou = drag(uo, un) * (un - uo)
        ov = drag(vo, vn) * (vn - vo)
        for j in range(CH):
            b, r = c // SUB, c % SUB + j
            at = pl.ds(r, rows, stride=SUB)
            res_v[0, b, at, :] = un[j]
            res_v[1, b, at, :] = vn[j]
            res_s[0, b, at, :] = sr1[j]
            res_s[1, b, at, :] = sr2[j]
            res_s[2, b, at, :] = s12[j + 1]
            res_o[0, b, at, :] = ou[j]
            res_o[1, b, at, :] = ov[j]

    lane_m = lax.broadcasted_iota(jnp.int32, (mrows, LANES), 1)
    m_last = lane_m == LANES - 1

    def m_west(x):
        return pltpu.roll(x, 1, 0)

    def m_east(x):
        return pltpu.roll(x, mrows - 1, 0)

    def m_down(x):
        return pltpu.roll(x, 1, 1)

    def m_up(x, ghost):
        return jnp.where(m_last, ghost, pltpu.roll(x, LANES - 1, 1))

    def m_prepare():
        whole = MP[...]
        raw = [
            whole if (LANES - SUB - SUB * f) % LANES == 0
            else pltpu.roll(whole, (LANES - SUB - SUB * f) % LANES, 1)
            for f in range(12)
        ]
        u, v, s1, s2, s12, uo, vo, tx, ty, conc, thick, kind = raw
        MV[0, 0], MV[0, 1] = u, v
        MS[0], MS[1], MS[2] = s1, s2, s12
        for f, value in enumerate(statics(conc, thick, kind, u, v, tx, ty, uo, vo)):
            MST[f] = value
        MST[7] = uo
        MST[8] = vo

    def m_stress(k):
        u, v = MV[k, 0], MV[k, 1]
        up, vp = m_up(u, -G[k, 0]), m_up(v, -G[k, 1])
        um, vm = m_down(u), m_down(v)
        du = u - m_west(u)
        dup = up - m_west(up)
        dv = v - vm
        dvp = vp - v
        div, ten = du + dv, du - dv
        dsum, tsum = div + (dup + dvp), ten + (dup - dvp)
        shear = (up - u) + (m_east(v) - v)
        ssum = shear + ((u - um) + (m_east(vm) - vm))
        src = 3 * k
        got = stress_rule(
            MS[src], MS[src + 1], MS[src + 2], div, ten, ssum + m_west(ssum),
            dsum + m_east(dsum), tsum + m_east(tsum), shear, MST[0], MST[1],
        )
        for f in range(3):
            MS[src + 3 + f] = got[f]
        MN[...] = got[0] - got[1]

    def m_vel(k):
        src = 3 * k + 3
        s1, s2, s12 = MS[src], MS[src + 1], MS[src + 2]
        n11, n22 = s1 + s2, s1 - s2
        u, v = MV[k, 0], MV[k, 1]
        up, vm = m_up(u, -G[k, 0]), m_down(v)
        fu = 0.5 * (m_east(n11) - n11) + (s12 - m_down(s12))
        fv = 0.5 * (m_up(n22, GN[k]) - n22) + (s12 - m_west(s12))
        va, ua = v + vm, u + up
        f = 0.25 * cor[rows - 1 : rows, :]
        MV[k + 1, 0] = vel_rule(
            u, MST[3], fu, MST[7], MST[2], f * (va + m_east(va)), MST[1], MST[5]
        )
        MV[k + 1, 1] = vel_rule(
            v, MST[4], fv, MST[8], MST[2], -f * (ua + m_west(ua)), MST[1], MST[6]
        )

    to_mirror.wait_recv()

    @pl.when(mir_l != me)
    def _():
        to_ml.wait_recv()

    @pl.when(mir_l == me)
    def _():
        MP[0:SUB, :] = tile[cols - SUB : cols, :]

    @pl.when(mir_r != me)
    def _():
        to_mr.wait_recv()

    @pl.when(mir_r == me)
    def _():
        MP[SUB + cols : mrows, :] = tile[0:SUB, :]

    m_prepare()

    def run(part, body):
        if len(part) == 3:
            pairs(*part, body)
        else:
            loop(*part, body)

    def sweep(start_parts, stress_parts, vel_parts):
        for lo, hi in start_parts:
            loop(lo, hi, shift_start)
        for k in range(len(stress_parts)):
            m_stress(k)
            for part in stress_parts[k]:
                run(part, functools.partial(stress_step, k))
            if k + 1 < ITERS:
                m_vel(k)
                for part in vel_parts[k]:
                    run(part, functools.partial(vel_step, k))

    inner = (1, 4, 6)
    inner_vel = (3, 5, 8)
    sweep(
        [(0, cols)],
        [[(a, cols - a)] for a in inner],
        [[(a, cols - a)] for a in inner_vel],
    )

    for c in sends:
        c.wait_recv()

    pairs(-VEL_HALO, cols, VEL_HALO // CH, shift_start)
    edge = REST_HALO + 1
    pairs(-edge, cols, edge // CH, prepare)

    def both(reach, a):
        return [(-reach, cols - a, (reach + a) // CH)]

    sweep(
        [],
        [both(r, a) for r, a in zip(STRESS_REACH[:3], inner)]
        + [[(-STRESS_REACH[3], cols + STRESS_REACH[3])]],
        [both(r, a) for r, a in zip(VEL_REACH[:2], inner_vel)]
        + [[(-VEL_REACH[2], cols + VEL_REACH[2])]],
    )

    outs = []
    for b in range(cols // SUB):
        for c in range(b * SUB, (b + 1) * SUB, 2 * CH):
            vel_step(ITERS - 1, [c, c + CH])
        for t, (src, dst) in enumerate(((res_v, out_vel), (res_s, out_stress), (res_o, out_ocean))):
            outs.append(
                pltpu.make_async_copy(src.at[:, b], dst.at[:, b], out_sem.at[3 * b + t])
            )
            outs[-1].start()

    to_mirror.wait_send()

    @pl.when(mir_l != me)
    def _():
        to_ml.wait_send()

    @pl.when(mir_r != me)
    def _():
        to_mr.wait_send()

    for c in sends:
        c.wait_send()
    for c in outs:
        c.wait()


def to_tiles(x):
    lead, (c, r) = x.shape[:-2], x.shape[-2:]
    x = x.reshape(lead + (c // SUB, SUB, r // LANES, LANES))
    return jnp.swapaxes(x, -3, -2).reshape(lead + (c // SUB, r // LANES * SUB, LANES))


def from_tiles(x, c, r):
    lead = x.shape[:-3]
    x = x.reshape(lead + (c // SUB, r // LANES, SUB, LANES))
    return jnp.swapaxes(x, -3, -2).reshape(lead + (c, r))


def on_device(n_gx, n_gy, forcing, ice_state, velocity, stress, ice_mask):
    cols, height = ice_mask.shape
    rows = height // LANES
    blocks = cols // SUB
    width = cols + 2 * OFF
    f32 = jnp.float32

    def tiles(n):
        return (n, blocks, rows * SUB, LANES)

    def vmem(*shape):
        return pltpu.VMEM(shape, f32)

    mrows = cols + 2 * SUB
    dma = pltpu.SemaphoreType.DMA
    scratch = [
        vmem(*tiles(4)), vmem(*tiles(2)), vmem(*tiles(2)), vmem(*tiles(3)),
        pltpu.VMEM(tiles(1)[1:], jnp.int32),
        vmem(*tiles(2)), vmem(*tiles(3)), vmem(*tiles(2)),
        vmem(ITERS, 2, width, rows, LANES),
        vmem(ITERS + 1, 3, width, rows, LANES),
        vmem(7, width, rows, LANES),
        vmem(7, width, rows, LANES),
        vmem(ITERS, 2, width, rows, LANES),
        vmem(ITERS, 2, width, rows, LANES),
        vmem(ITERS, width, rows, LANES),
        vmem(ITERS, width, rows, LANES),
        vmem(rows, LANES),
        vmem(cols, LANES),
        vmem(mrows, LANES),
        vmem(ITERS, 2, mrows, LANES),
        vmem(3 * (ITERS + 1), mrows, LANES),
        vmem(9, mrows, LANES),
        vmem(mrows, LANES),
        vmem(ITERS, 2, mrows, LANES),
        vmem(ITERS, mrows, LANES),
        dma((5,)), dma((3 * blocks,)), dma((6,)), dma((6,)), dma((3,)), dma((3,)),
    ]
    any_spec = pl.BlockSpec(memory_space=pl.ANY)
    vel, str_, ocean = pl.pallas_call(
        functools.partial(kernel, n_gx, n_gy),
        out_shape=[jax.ShapeDtypeStruct(tiles(n), f32) for n in (2, 3, 2)],
        in_specs=[any_spec] * 5,
        out_specs=[any_spec] * 3,
        scratch_shapes=scratch,
        compiler_params=pltpu.CompilerParams(
            collective_id=0, has_side_effects=True, vmem_limit_bytes=60 * 1024 * 1024
        ),
    )(to_tiles(forcing), to_tiles(ice_state), to_tiles(velocity), to_tiles(stress), to_tiles(ice_mask))
    return (
        from_tiles(vel, cols, height),
        from_tiles(str_, cols, height),
        from_tiles(ocean, cols, height),
    )


def solution(mesh):
    spec = P(None, ("gx", "gy"), None)
    return jax.shard_map(
        functools.partial(on_device, mesh.shape["gx"], mesh.shape["gy"]),
        mesh=mesh,
        in_specs=(spec, spec, spec, spec, P(("gx", "gy"), None)),
        out_specs=(spec, spec, spec),
        check_vma=False,
    )
```
